128 devices in a mesh: dp: 16 (over y_hi, x, core), tensor: 8 (over z, y_lo).
Axes of the slice: x: 4, y: 4 (y_hi: 2, y_lo: 2; y = y_hi * 2 + y_lo), z: 4, core: 2. Of those that a mesh axis runs over, the one named last changes fastest.
Arguments:
- tokens: bfloat16 [32768, 1024], P(('dp', 'tensor')), may hold values from -6 to 6
- upstream: bfloat16 [32768, 1024], P(('dp', 'tensor')), may hold values from -6 to 6
- counts: int32 [512], P('dp'), may hold values from 37 to 49, as said below
- norm_gain: float32 [1024], replicated, may hold values from 0.5 to 1.5
- norm_bias: float32 [1024], replicated, may hold values from -4 to 4
- w_qkv: bfloat16 [1024, 3072], P('dp', 'tensor'), may hold values from -0.1875 to 0.1875
- w_out: bfloat16 [1024, 1024], P('tensor', 'dp'), may hold values from -0.1875 to 0.1875
Outputs:
- grad_tokens: bfloat16 [32768, 1024], P(('dp', 'tensor'))
- grad_qkv: float32 [1024, 3072], P('dp', 'tensor')
- grad_out: float32 [1024, 1024], P('tensor', 'dp')
- grad_gain: float32 [1024], replicated
- grad_bias: float32 [1024], replicated
The draws below stay inside these ranges and needn't reach their ends.
Inputs may be any that keep to these rules, and one draw needn't show every extreme that they name: counts[i] is the number of visible tokens of image i, held in its first slots; some image has 49 in every draw.
All inputs are finite; a program needn't handle non-finite values.
Results may differ from the reference program's by a relative error of at most 0.014.
Values may be sent and summed in bfloat16 or wider, within the bound.
No kernel may reach another device: no remote copies, remote signals or barrier semaphores. Data moves between devices by JAX's collectives and lax.ppermute only.
A program may use at most 64 MiB of HBM per device.

```python
import jax
import jax.numpy as jnp
from jax import lax

D = 1024
HEADS = 16
HEAD = 64
CAP = 64
MAXC = 49
MINC = 37
IMAGES = 512
TOKENS = 32768


def draw_counts(key, part):
    values = jax.random.randint(key, (IMAGES,), MINC, MAXC + 1, dtype=jnp.int32)
    position = jax.random.randint(jax.random.fold_in(key, 17), (), 0, IMAGES, dtype=jnp.int32)
    return values.at[position].set(MAXC)


def levels(stream_key, dims, cuts, low, high):
    factor_of = 1.0
    for dim, parts in cuts:
        draws = jax.random.uniform(jax.random.fold_in(jax.random.fold_in(stream_key, 6), dim), (parts,), jnp.float32, low / len(cuts), high / len(cuts))
        factor_of = factor_of * jnp.repeat(jnp.exp(draws), dims[dim] // parts).reshape((-1,) + (1,) * (len(dims) - 1 - dim))
    return factor_of


def noise(own_key, extent, scale, reach, cuts=(), kind=jnp.bfloat16):
    loudness = levels(own_key, extent, cuts, -0.22, 0.18) if cuts else 1.0
    values = jax.random.normal(own_key, extent, jnp.float32) * scale * loudness
    return jnp.minimum(jnp.maximum(values, -reach), reach).astype(kind)


def setup_inputs(seed: int = 0) -> dict:
    splits = jax.random.split(jax.random.key(seed), 8)
    return {
        "tokens": noise(splits[0], (TOKENS, D), 1.0, 6.0, ((0, 128),)),
        "upstream": noise(splits[1], (TOKENS, D), 1.0, 6.0, ((0, 128),)),
        "counts": draw_counts(jax.random.fold_in(splits[7], 71), 0),
        "norm_gain": jnp.clip(1.0 + 0.1 * jax.random.normal(splits[3], (D,), jnp.float32), 0.5, 1.5),
        "norm_bias": noise(splits[4], (D,), 1.0, 4.0, (), jnp.float32),
        "w_qkv": noise(splits[5], (D, 3 * D), D ** -0.5, 0.1875, ((0, 16), (1, 8))),
        "w_out": noise(splits[6], (D, D), D ** -0.5, 0.1875, ((0, 8), (1, 16))),
    }


def layer_norm(tokens, norm_gain, norm_bias):
    values = tokens.astype(jnp.float32)
    centre = lax.optimization_barrier(jnp.mean(values, axis=-1, keepdims=True))
    shifted = values - centre
    variance = lax.optimization_barrier(jnp.mean(shifted * shifted, axis=-1, keepdims=True))
    inverse_std = lax.rsqrt(variance + 1e-06)
    scaled = shifted * inverse_std
    normed = (scaled * norm_gain + norm_bias).astype(jnp.bfloat16)
    return (normed, scaled, inverse_std)

def reference(tokens, upstream, counts, norm_gain, norm_bias, w_qkv, w_out):
    total = tokens.shape[0]
    images = total // CAP
    slot_live = jnp.arange(CAP, dtype=jnp.int32)[None, :] < counts[:, None]
    live = slot_live.reshape(-1).astype(jnp.float32)
    normed, scaled, inverse_std = layer_norm(tokens, norm_gain, norm_bias)
    projected = jnp.dot(normed, w_qkv, preferred_element_type=jnp.float32).astype(jnp.bfloat16)
    projected = projected.reshape(images, CAP, HEADS, 3, HEAD)
    query_rows = projected[:, :, :, 0].astype(jnp.float32)
    key_rows = projected[:, :, :, 1].astype(jnp.float32)
    value_rows = projected[:, :, :, 2].astype(jnp.float32)
    score_scale = 1.0 / HEAD ** 0.5
    scores = jnp.einsum('bqhe,bkhe->bhqk', query_rows, key_rows) * score_scale
    scores = jnp.where(slot_live[:, None, None, :], scores, -1e+30)
    probs = jax.nn.softmax(scores, axis=-1)
    probs_low = probs.astype(jnp.bfloat16).astype(jnp.float32)
    attended = jnp.einsum('bhqk,bkhe->bqhe', probs_low, value_rows).astype(jnp.bfloat16).reshape(total, D)
    masked = (upstream.astype(jnp.float32) * live[:, None]).astype(jnp.bfloat16)
    grad_out = lax.dot_general(attended, masked, (((0,), (0,)), ((), ())), preferred_element_type=jnp.float32)
    grad_att = lax.dot_general(masked, w_out, (((1,), (1,)), ((), ())), preferred_element_type=jnp.float32)
    grad_att = grad_att.astype(jnp.bfloat16).reshape(images, CAP, HEADS, HEAD).astype(jnp.float32)
    grad_probs = jnp.einsum('bqhe,bkhe->bhqk', grad_att, value_rows)
    row_delta = lax.optimization_barrier(jnp.sum(probs * grad_probs, axis=-1, keepdims=True))
    grad_scores = (probs * (grad_probs - row_delta) * score_scale).astype(jnp.bfloat16).astype(jnp.float32)
    grad_value = jnp.einsum('bhqk,bqhe->bkhe', probs_low, grad_att).astype(jnp.bfloat16)
    grad_query = jnp.einsum('bhqk,bkhe->bqhe', grad_scores, key_rows).astype(jnp.bfloat16)
    grad_key = jnp.einsum('bhqk,bqhe->bkhe', grad_scores, query_rows).astype(jnp.bfloat16)
    grad_proj = jnp.stack([grad_query, grad_key, grad_value], axis=3).reshape(total, 3 * D)
    grad_qkv = lax.dot_general(normed, grad_proj, (((0,), (0,)), ((), ())), preferred_element_type=jnp.float32)
    grad_normed = lax.dot_general(grad_proj, w_qkv, (((1,), (1,)), ((), ())), preferred_element_type=jnp.float32)
    grad_gain = lax.optimization_barrier(jnp.sum(grad_normed * scaled, axis=0))
    grad_bias = lax.optimization_barrier(jnp.sum(grad_normed, axis=0))
    grad_scaled = grad_normed * norm_gain
    grad_ln = inverse_std * (grad_scaled - lax.optimization_barrier(jnp.mean(grad_scaled, axis=-1, keepdims=True)) - scaled * lax.optimization_barrier(jnp.mean(grad_scaled * scaled, axis=-1, keepdims=True)))
    grad_tokens = (upstream.astype(jnp.float32) * live[:, None] + grad_ln).astype(jnp.bfloat16)
    return (grad_tokens, grad_qkv, grad_out, grad_gain, grad_bias)
```

```python
import jax
import jax.numpy as jnp
from jax import lax
from jax.experimental import pallas as pl
from jax.experimental.pallas import tpu as pltpu
from jax.sharding import Mesh
from jax.sharding import PartitionSpec as P

HEAD = 64
CAP = 64
MAXC = 49
IMGS = 4
ROWS = 208
MASK_ROW = 200
D = 1024
BLK = 64
WIDE = 512
AXES = ("y_hi", "x", "core", "z", "y_lo")
DP = ("y_hi", "x", "core")
TENSOR = ("z", "y_lo")
PLANE = ("y_lo", "y_hi", "x")
F32 = jnp.float32
BF16 = jnp.bfloat16
VMEM = pl.BlockSpec(memory_space=pltpu.VMEM)
SMEM = pl.BlockSpec(memory_space=pltpu.SMEM)


def ring(n, k):
    return [(i, (i + k) % n) for i in range(n)]


def nn(a, b):
    return lax.dot_general(a, b, (((1,), (0,)), ((), ())), preferred_element_type=F32)


def nt(a, b):
    return lax.dot_general(a, b, (((1,), (1,)), ((), ())), preferred_element_type=F32)


def tn(a, b):
    return lax.dot_general(a, b, (((0,), (0,)), ((), ())), preferred_element_type=F32)


def image_of(index):
    return (
        (index >= MAXC).astype(jnp.int32)
        + (index >= 2 * MAXC).astype(jnp.int32)
        + (index >= 3 * MAXC).astype(jnp.int32)
    )


def count_of(image, counts):
    picked = jnp.where(image == 0, counts[0], counts[1])
    picked = jnp.where(image == 2, counts[2], picked)
    return jnp.where(image == 3, counts[3], picked)


def pack_kernel(start, counts, tokens, upstream, w_qkv, w_out, x_out, u_out, w_cat):
    own = [counts[start[0] + i] for i in range(IMGS)]
    row = lax.broadcasted_iota(jnp.int32, (ROWS, IMGS * CAP), 0)
    col = lax.broadcasted_iota(jnp.int32, (ROWS, IMGS * CAP), 1)
    image = image_of(row)
    slot = row - MAXC * image
    live = slot < count_of(image, own)
    pick = jnp.where(live & (col == CAP * image + slot), 1.0, 0.0).astype(BF16)
    x = nn(pick, tokens[...]).astype(BF16)
    u_out[...] = nn(pick, upstream[...]).astype(BF16)
    key = lax.broadcasted_iota(jnp.int32, (16, D), 1)
    key_image = image_of(key)
    key_slot = key - MAXC * key_image
    key_live = jnp.where(key_slot < count_of(key_image, own), 1.0, 0.0)
    at = lax.broadcasted_iota(jnp.int32, (16, D), 0) == MASK_ROW - (ROWS - 16)
    tail = jnp.where(at, key_live, 0.0).astype(BF16)
    x_out[0 : ROWS - 16] = x[0 : ROWS - 16]
    x_out[ROWS - 16 : ROWS] = x[ROWS - 16 : ROWS] + tail
    for head in range(2):
        for part in range(3):
            w_cat[:, (2 * part + head) * HEAD : (2 * part + head + 1) * HEAD] = w_qkv[
                :, (3 * head + part) * HEAD : (3 * head + part + 1) * HEAD
            ]
    w_cat[:, 6 * HEAD :] = w_out[...].astype(F32).T.astype(BF16)


def block_kernel(
    core, xa, xb, ua, ub, w_own, w_other, gain, bias, g_in, gb_in,
    gn_a, gn_b, g_out, gb_out,
    normed_s, xhat_s, u_s, w_s, *, first, last,
):
    c = core[0]
    for i in range(8):
        w_s[i, c] = w_own[c, i]
        w_s[i, 1 - c] = w_other[c, i]
    gain_row = gain[...]
    bias_row = bias[...]

    for s, (x_ref, u_ref) in enumerate(((xa, ua), (xb, ub))):
        def norm_rows(i, _, x_ref=x_ref, s=s):
            at = pl.multiple_of(i * 16, 16)
            values = x_ref[pl.ds(at, 16), :].astype(F32)
            centre = jnp.mean(values, axis=-1, keepdims=True)
            shifted = values - centre
            variance = jnp.mean(shifted * shifted, axis=-1, keepdims=True)
            scaled = shifted * lax.rsqrt(variance + 1e-06)
            to = pl.multiple_of(s * ROWS + i * 16, 16)
            xhat_s[pl.ds(to, 16), :] = scaled
            normed_s[pl.ds(to, 16), :] = (scaled * gain_row + bias_row).astype(BF16)
            return 0

        lax.fori_loop(0, ROWS // 16, norm_rows, 0)
        u_s[s * ROWS : (s + 1) * ROWS] = u_ref[...]

    weights = w_s[...].reshape(D, WIDE)
    w_proj = weights[:, : 6 * HEAD]
    w_back = weights[:, 6 * HEAD :]
    projected = nn(normed_s[...], w_proj).astype(BF16)
    grad_att = nn(u_s[...], w_back).astype(BF16)

    lane = lax.broadcasted_iota(jnp.int32, (1, 2 * HEAD), 1)
    zero = jnp.zeros((), BF16)
    q_image = jnp.minimum(image_of(lax.broadcasted_iota(jnp.int32, (ROWS, ROWS), 0)), 3)
    key = lax.broadcasted_iota(jnp.int32, (ROWS, ROWS), 1)
    same = (q_image == image_of(key)) & (key < IMGS * MAXC)

    attended_parts = []
    grad_parts = []
    for s, x_ref in enumerate((xa, xb)):
        lo, hi = s * ROWS, (s + 1) * ROWS
        q = projected[lo:hi, 0 : 2 * HEAD]
        k = projected[lo:hi, 2 * HEAD : 4 * HEAD]
        v = projected[lo:hi, 4 * HEAD : 6 * HEAD]
        da = grad_att[lo:hi]
        key_live = x_ref[ROWS - 16 : ROWS, 0:ROWS].astype(F32)[MASK_ROW - (ROWS - 16) : MASK_ROW - (ROWS - 16) + 1]
        keep = same & (key_live > 0.5)
        attended = None
        for head in range(2):
            mine = (lane < HEAD) if head == 0 else (lane >= HEAD)
            q_h = jnp.where(mine, q, zero)
            k_h = jnp.where(mine, k, zero)
            v_h = jnp.where(mine, v, zero)
            da_h = jnp.where(mine, da, zero)
            scores = jnp.where(keep, nt(q_h, k) * (1.0 / 8.0), -1e30)
            top = jnp.max(scores, axis=-1, keepdims=True)
            powers = jnp.exp(scores - top)
            probs = powers / jnp.sum(powers, axis=-1, keepdims=True)
            low = probs.astype(BF16)
            grad_probs = nt(da_h, v)
            delta = jnp.sum(probs * grad_probs, axis=-1, keepdims=True)
            grad_scores = (probs * (grad_probs - delta) * (1.0 / 8.0)).astype(BF16)
            att = nn(low, v_h)
            gv = tn(low, da_h)
            gq = nn(grad_scores, k_h)
            gk = tn(grad_scores, q_h)
            if attended is None:
                attended, grad_v, grad_q, grad_k = att, gv, gq, gk
            else:
                attended, grad_v, grad_q, grad_k = attended + att, grad_v + gv, grad_q + gq, grad_k + gk
        attended_parts.append(attended.astype(BF16))
        grad_parts.append(jnp.concatenate([grad_q, grad_k, grad_v], axis=1).astype(BF16))
    attended = jnp.concatenate(attended_parts, axis=0)
    grad_proj = jnp.concatenate(grad_parts, axis=0)

    qkv_part = tn(normed_s[...], grad_proj)
    out_part = tn(u_s[...], attended)
    if not first:
        qkv_part = qkv_part + g_in[:, : 6 * HEAD]
        out_part = out_part + g_in[:, 6 * HEAD :]
    if last:
        for part, at in ((qkv_part, 0), (out_part, 6 * HEAD)):
            part = part.astype(BF16).reshape(8, 2, BLK, -1)
            for half in range(2):
                g_out[half, :, :, at : at + part.shape[-1]] = part[:, half]
    else:
        g_out[:, : 6 * HEAD] = qkv_part
        g_out[:, 6 * HEAD :] = out_part
    grad_normed = nt(grad_proj, w_proj)
    gn_a[...] = grad_normed[:ROWS].astype(BF16)
    gn_b[...] = grad_normed[ROWS:].astype(BF16)
    gain_sum = jnp.sum(grad_normed * xhat_s[...], axis=0, keepdims=True)
    bias_sum = jnp.sum(grad_normed, axis=0, keepdims=True)
    sums = jnp.concatenate([gain_sum, bias_sum], axis=0)
    gb_out[...] = sums if first else gb_in[...] + sums


def finish_kernel(p0, p1, p2, p3, x_ref, u_ref, gain, out):
    grad_normed = (
        p0[...].astype(F32) + p1[...].astype(F32) + p2[...].astype(F32) + p3[...].astype(F32)
    )
    values = x_ref[...].astype(F32)
    centre = jnp.mean(values, axis=-1, keepdims=True)
    shifted = values - centre
    variance = jnp.mean(shifted * shifted, axis=-1, keepdims=True)
    inverse_std = lax.rsqrt(variance + 1e-06)
    scaled = shifted * inverse_std
    g = grad_normed * gain[...]
    grad_ln = inverse_std * (
        g
        - jnp.mean(g, axis=-1, keepdims=True)
        - scaled * jnp.mean(g * scaled, axis=-1, keepdims=True)
    )
    packed = (u_ref[...].astype(F32) + grad_ln).astype(BF16)
    row = lax.broadcasted_iota(jnp.int32, (IMGS * CAP, ROWS), 0)
    col = lax.broadcasted_iota(jnp.int32, (IMGS * CAP, ROWS), 1)
    slot = row % CAP
    pick = jnp.where((slot < MAXC) & (col == MAXC * (row // CAP) + slot), 1.0, 0.0).astype(BF16)
    out[...] = nn(pick, packed).astype(BF16)


def weights_kernel(arrived, qkv_out, out_out):
    total = jnp.sum(arrived[...].astype(F32), axis=0)
    for head in range(2):
        for part in range(3):
            qkv_out[:, (3 * head + part) * HEAD : (3 * head + part + 1) * HEAD] = total[
                :, (2 * part + head) * HEAD : (2 * part + head + 1) * HEAD
            ]
    out_out[...] = total[:, 6 * HEAD :].T


def shape(dims, kind=BF16):
    return jax.ShapeDtypeStruct(dims, kind)


def swap(value):
    return lax.ppermute(value, "core", ring(2, 1))


def on_device(tokens, upstream, counts, norm_gain, norm_bias, w_qkv, w_out):
    core = lax.axis_index("core").astype(jnp.int32).reshape(1)
    start = (lax.axis_index(TENSOR) * IMGS).astype(jnp.int32).reshape(1)
    gain = norm_gain.reshape(1, D)
    bias = norm_bias.reshape(1, D)
    x, u, w_cat = pl.pallas_call(
        pack_kernel,
        in_specs=[SMEM, SMEM, VMEM, VMEM, VMEM, VMEM],
        out_specs=[VMEM, VMEM, VMEM],
        out_shape=[shape((ROWS, D)), shape((ROWS, D)), shape((BLK, WIDE))],
        name="pack",
    )(start, counts, tokens, upstream, w_qkv, w_out)

    xs = [x] + [lax.ppermute(x, "z", ring(4, k)) for k in (1, 2, 3)]
    us = [u] + [lax.ppermute(u, "z", ring(4, k)) for k in (1, 2, 3)]
    copies = jnp.broadcast_to(w_cat, (16, BLK, WIDE))
    w_own = lax.all_to_all(copies, PLANE, 0, 0, tiled=True).reshape(2, 8, BLK, WIDE)
    w_other = swap(w_own)

    order = (0, 1, 3, 2)
    partial = {}
    grads = jnp.zeros((8, 128), F32)
    sums = jnp.zeros((2, D), F32)
    for step, k in enumerate(order):
        first, last = step == 0, step == 3
        g_shape = shape((2, 8, BLK, WIDE)) if last else shape((D, WIDE), F32)

        def kernel(*refs, first=first, last=last):
            block_kernel(*refs, first=first, last=last)

        gn_a, gn_b, grads, sums = pl.pallas_call(
            kernel,
            in_specs=[SMEM] + [VMEM] * 10,
            out_specs=[VMEM] * 4,
            out_shape=[shape((ROWS, D)), shape((ROWS, D)), g_shape, shape((2, D), F32)],
            scratch_shapes=[
                pltpu.VMEM((2 * ROWS, D), BF16),
                pltpu.VMEM((2 * ROWS, D), F32),
                pltpu.VMEM((2 * ROWS, D), BF16),
                pltpu.VMEM((8, 2, BLK, WIDE), BF16),
            ],
            name=f"block{k}",
        )(core, xs[k], swap(xs[k]), us[k], swap(us[k]), w_own, w_other, gain, bias, grads, sums)
        pair = (gn_a.astype(F32) + swap(gn_b).astype(F32)).astype(BF16)
        partial[k] = lax.ppermute(pair, "z", ring(4, 4 - k)) if k else pair

    other = swap(grads)
    here = core[0] == 0
    send = jnp.stack(
        [jnp.where(here, grads[0], other[1]), jnp.where(here, other[0], grads[1])]
    ).reshape(16, BLK, WIDE)
    arrived = lax.all_to_all(send, PLANE, 0, 0, tiled=True)

    for axis, n, k in (
        ("core", 2, 1), ("y_lo", 2, 1), ("z", 4, 2), ("z", 4, 1), ("x", 4, 2), ("x", 4, 1), ("y_hi", 2, 1)
    ):
        sums = sums + lax.ppermute(sums, axis, ring(n, k))

    grad_qkv, grad_out = pl.pallas_call(
        weights_kernel,
        in_specs=[VMEM],
        out_specs=[VMEM, VMEM],
        out_shape=[shape((BLK, 6 * HEAD), F32), shape((2 * HEAD, BLK), F32)],
        name="weights",
    )(arrived)
    grad_tokens = pl.pallas_call(
        finish_kernel,
        in_specs=[VMEM] * 7,
        out_specs=VMEM,
        out_shape=shape((IMGS * CAP, D)),
        name="finish",
    )(partial[0], partial[1], partial[2], partial[3], x, u, gain)
    return (grad_tokens, grad_qkv, grad_out, sums[0], sums[1])


def solution(mesh):
    finer = Mesh(mesh.devices.reshape(2, 4, 2, 4, 2), AXES)
    rows = DP + TENSOR
    in_specs = (P(rows, None), P(rows, None), P(DP), P(), P(), P(DP, TENSOR), P(TENSOR, DP))
    out_specs = (P(rows, None), P(DP, TENSOR), P(TENSOR, DP), P(), P())
    return jax.shard_map(
        on_device, mesh=finer, in_specs=in_specs, out_specs=out_specs, check_vma=False
    )
```
